32 devices in a mesh: rows: 16 (over z, y, x), spec: 2 (over core).
Axes of the slice: x: 2, y: 2, z: 4, core: 2. Of those that a mesh axis runs over, the one named last changes fastest.
Arguments:
- field: float32 [36, 30, 8192], P('spec', None, 'rows'), may hold values from 0.1 to 4
- group_speed: float32 [30], replicated, may hold values from 0.3 to 1
- face_angle: float32 [16384], P('rows'), may hold values from -3.140625 to 3.140625
- face_speed: float32 [16384], P('rows'), may hold values from 0.04 to 0.2
- face_cells: int32 [2, 16384], P(None, 'rows'), may hold values from 0 to 1023, as said below
- face_live: int32 [16], P('rows'), may hold values from 1 to 8, as said below
- halo_blocks: int32 [16, 2, 2], P('rows'), may hold values from 0 to 3
- cell_level: int32 [8192], P('rows'), may hold values from 0 to 2
- polar_mask: int32 [8192], P('rows'), may hold values 0 or 1
- turn_rate: float32 [8192], P('rows'), may hold values from -0.45 to 0.45
Outputs:
- advanced: float32 [36, 30, 8192], P('spec', None, 'rows')
The draws below stay inside these ranges and needn't reach their ends.
Inputs may be any that keep to these rules, and one draw needn't show every extreme that they name: `face_cells`: row 0 is a face's lower cell, a position among its row block's own 512 cells; row 1 its upper cell, a position among the own cells followed by 2 halo blocks from the block before and 2 from the block after (128 cells each). Only the first face_live[r] of row block r's 8 face blocks carry faces; some row block has all 8 live.
All inputs are finite; a program needn't handle non-finite values. No bound on the sum of `polar_mask` on one device may be relied on, other than what follows from the above.
Results may differ from the reference program's by a relative error of at most 0.0003.
Values sent between devices are 32-bit elements; how exact they have to be, the bound alone decides.
A program may use at most 64 MiB of HBM per device.

```python
import math
import jax
import jax.numpy as jnp
from jax import lax

NDIR = 36
NFREQ = 30
CELL_DEV = 512
HBO = 2
ITERS = 3
FBLK = 8
CELLS = 8192
FACES = 16384
N_ROWS = 16


def draw_face_cells(key, part):
    base = jax.random.fold_in(key, 11)
    key_low, key_own, key_halo, key_pick = jax.random.split(base, 4)
    faces = N_ROWS * FBLK * 128
    lower = jax.random.randint(key_low, (faces,), 0, CELL_DEV)
    own_upper = jax.random.randint(key_own, (faces,), 0, CELL_DEV)
    halo_upper = CELL_DEV + jax.random.randint(key_halo, (faces,), 0, 256 * HBO)
    picked = jax.random.randint(key_pick, (faces,), 0, 100) < 20
    upper = jnp.where(picked, halo_upper, own_upper)
    return jnp.stack([lower, upper]).astype(jnp.int32)


def draw_face_live(key, part):
    base = jax.random.fold_in(key, 23)
    key_first, key_second, key_full = jax.random.split(base, 3)
    first = jax.random.randint(key_first, (N_ROWS,), 0, FBLK + 1)
    second = jax.random.randint(key_second, (N_ROWS,), 0, FBLK + 1)
    live = jnp.maximum(1, first * second // FBLK)
    fullest = jax.random.randint(key_full, (), 0, N_ROWS)
    return live.at[fullest].set(FBLK).astype(jnp.int32)


def touch_ends(array, own_key, low, high):
    dims = array.shape
    spot = [jax.random.randint(jax.random.fold_in(own_key, axis), (), 0, dims[axis]) for axis in range(len(dims))]
    array = array.at[tuple(spot)].set(low)
    longest = dims.index(max(dims))
    spot[longest] = (spot[longest] + 1) % dims[longest]
    return array.at[tuple(spot)].set(high)


def block_levels(rng, shape, pieces, least, largest):
    def one(axis_at, parts):
        heights = jax.random.uniform(jax.random.fold_in(jax.random.fold_in(rng, 6), axis_at), (parts,), jnp.float32, least / len(pieces), largest / len(pieces))
        return jnp.repeat(jnp.exp(heights), shape[axis_at] // parts).reshape((-1,) + (1,) * (len(shape) - axis_at - 1))

    loudness = one(*pieces[0])
    for cut in pieces[1:]:
        loudness = loudness * one(*cut)
    return loudness


def setup_inputs(seed: int = 0) -> dict:
    arg_keys = jax.random.split(jax.random.key(seed), 11)
    field = jnp.clip(jnp.exp(math.log(4.0) - 3.6888794 * jax.random.uniform(arg_keys[0], (NDIR, NFREQ, CELLS), jnp.float32) ** block_levels(arg_keys[0], (NDIR, NFREQ, CELLS), ((0, 2), (2, 16)), -0.2, 0.2)), 0.1, 4.0)
    group_speed = jnp.clip(jnp.exp(jax.random.uniform(arg_keys[1], (NFREQ,), jnp.float32, math.log(0.3), math.log(1.0))), 0.3, 1.0)
    face_angle = jnp.clip(jax.random.uniform(arg_keys[2], (FACES,), jnp.float32, -3.140625, 3.140625), -3.140625, 3.140625)
    face_speed = jnp.clip(jnp.exp(math.log(0.2) - 1.609438 * jax.random.uniform(arg_keys[3], (FACES,), jnp.float32) ** block_levels(arg_keys[3], (FACES,), ((0, 16),), -0.2, 0.2)), 0.04, 0.2)
    face_cells = draw_face_cells(jax.random.fold_in(arg_keys[10], 71), 0)
    face_live = draw_face_live(jax.random.fold_in(arg_keys[10], 71), 0)
    halo_blocks = touch_ends(jax.random.randint(arg_keys[6], (N_ROWS, 2, HBO), 0, CELL_DEV // 128), jax.random.fold_in(arg_keys[6], 1), 0, (CELL_DEV // 128) - 1).astype(jnp.int32)
    cell_level = touch_ends(jax.random.randint(arg_keys[7], (CELLS,), 0, 3), jax.random.fold_in(arg_keys[7], 1), 0, 2).astype(jnp.int32)
    polar_mask = touch_ends((jax.random.randint(arg_keys[8], (CELLS,), 0, 3) < 1).astype(jnp.int32), jax.random.fold_in(arg_keys[8], 1), 0, 1)
    turn_rate = jnp.clip(jax.random.uniform(arg_keys[9], (CELLS,), jnp.float32, -0.45, 0.45) * block_levels(arg_keys[9], (CELLS,), ((0, 16),), -0.4, 0.0), -0.45, 0.45)
    return {"field": field, "group_speed": group_speed, "face_angle": face_angle, "face_speed": face_speed, "face_cells": face_cells, "face_live": face_live, "halo_blocks": halo_blocks, "cell_level": cell_level, "polar_mask": polar_mask, "turn_rate": turn_rate}


def face_flux_sum(total, ext, lower, upper, weight, theta, angle, group_speed):
    cosine = jnp.cos(theta[:, None] - angle[None, :]) * weight[None, :]
    velocity = group_speed[None, :, None] * cosine[:, None, :]
    low_vals = jnp.take(ext, lower, axis=2)
    up_vals = jnp.take(ext, upper, axis=2)
    flux = jnp.maximum(velocity, 0.0) * low_vals + jnp.minimum(velocity, 0.0) * up_vals
    total = total.at[:, :, lower].add(flux)
    return total.at[:, :, upper].add(-flux)


def pick_blocks(neighbour, table):
    ndir, nfreq, cdev = neighbour.shape
    view = neighbour.reshape(ndir, nfreq, cdev // 128, 128)
    return jnp.take(view, table, axis=2).reshape(ndir, nfreq, -1)


def reference(field, group_speed, face_angle, face_speed, face_cells, face_live, halo_blocks, cell_level, polar_mask, turn_rate):
    ndir, nfreq, cells = field.shape
    rows_n = N_ROWS
    cdev = cells // rows_n
    fdev = face_angle.shape[0] // rows_n
    theta = (jnp.arange(ndir, dtype=jnp.float32) + 0.5) * (2.0 * math.pi / NDIR)
    weight_turn = (polar_mask.astype(jnp.float32) * turn_rate)[None, None, :]
    current = field
    for step in range(ITERS):
        def one_row(r):
            own = lax.dynamic_slice_in_dim(current, r * cdev, cdev, 2)
            below = lax.dynamic_slice_in_dim(current, jnp.maximum(r - 1, 0) * cdev, cdev, 2) * (r > 0).astype(jnp.float32)
            above = lax.dynamic_slice_in_dim(current, jnp.minimum(r + 1, rows_n - 1) * cdev, cdev, 2) * (r < rows_n - 1).astype(jnp.float32)
            table = halo_blocks[r]
            ext = jnp.concatenate([own, pick_blocks(below, table[0]), pick_blocks(above, table[1])], axis=2)
            pair = lax.dynamic_slice_in_dim(face_cells, r * fdev, fdev, 1)
            angle = lax.dynamic_slice_in_dim(face_angle, r * fdev, fdev, 0)
            speed = lax.dynamic_slice_in_dim(face_speed, r * fdev, fdev, 0)
            live = (jnp.arange(fdev, dtype=jnp.int32) < face_live[r] * 128).astype(jnp.float32)
            total = jnp.zeros(ext.shape, jnp.float32)
            total = face_flux_sum(total, ext, pair[0], pair[1], speed * live, theta, angle, group_speed)
            level = lax.dynamic_slice_in_dim(cell_level, r * cdev, cdev, 0)
            return own - total[:, :, :cdev] * jnp.exp2(-level.astype(jnp.float32))[None, None, :]

        moved = lax.map(one_row, jnp.arange(rows_n, dtype=jnp.int32))
        moved = jnp.transpose(moved, (1, 2, 0, 3)).reshape(ndir, nfreq, cells)
        before = jnp.roll(moved, 1, axis=0)
        after = jnp.roll(moved, -1, axis=0)
        current = moved - jnp.maximum(weight_turn, 0.0) * (moved - before) - jnp.minimum(weight_turn, 0.0) * (after - moved)
    return current
```

```python
import math

import jax
import jax.numpy as jnp
from jax import lax
from jax.sharding import PartitionSpec as P

NDIR = 36
ITERS = 3


def with_halo(x, sides, width, wrap):
    for axis, dim in sides:
        size, length = (lax.axis_size(axis), x.shape[dim])
        up = [(i, (i + 1) % size) for i in range(size if wrap else size - 1)]
        down = [(j, i) for i, j in up]
        last = lax.slice_in_dim(x, length - width, length, axis=dim)
        first = lax.slice_in_dim(x, 0, width, axis=dim)
        before = lax.ppermute(last, axis, up)
        after = lax.ppermute(first, axis, down)
        x = jnp.concatenate([before, x, after], axis=dim)
    return x


def from_behind(value, axis, steps):
    count = lax.axis_size(axis)
    first, last = (max(0, -steps), min(count, count - steps))
    return lax.ppermute(value, axis, [(source, source + steps) for source in range(first, last)])


def pick_blocks(neighbour, table):
    ndir, nfreq, cdev = neighbour.shape
    view = neighbour.reshape(ndir, nfreq, cdev // 128, 128)
    return jnp.take(view, table, axis=2).reshape(ndir, nfreq, -1)


def split(x):
    high = x.astype(jnp.bfloat16)
    low = (x - high.astype(jnp.float32)).astype(jnp.bfloat16)
    return jnp.concatenate([high, low], axis=1)


def pieces_dot(x, hot, contract):
    return lax.dot_general(
        split(x), hot, (((1,), (contract,)), ((), ())), preferred_element_type=jnp.float32
    )


def block_flux(spectra, own_cells, own_hot, up_hot, signed_hot, forward, backward):
    low_vals = pieces_dot(spectra[:, :own_cells], own_hot, 0)
    up_vals = pieces_dot(spectra, up_hot, 0)
    flux = forward * low_vals + backward * up_vals
    return pieces_dot(flux, signed_hot, 1)


def on_device(
    field,
    group_speed,
    face_angle,
    face_speed,
    face_cells,
    face_live,
    halo_blocks,
    cell_level,
    polar_mask,
    turn_rate,
):
    dloc, nfreq, cdev = field.shape
    fdev = face_angle.shape[0]
    first_dir = lax.axis_index("spec") * dloc
    theta = ((first_dir + jnp.arange(dloc, dtype=jnp.int32)).astype(jnp.float32) + 0.5) * (
        2.0 * math.pi / NDIR
    )
    weight_turn = (polar_mask.astype(jnp.float32) * turn_rate)[None, None, :]
    area_scale = jnp.exp2(-cell_level.astype(jnp.float32))[None, None, :]
    live_count = face_live[0]
    slot_live = (jnp.arange(fdev, dtype=jnp.int32) < live_count * 128).astype(jnp.float32)
    slot_weight = face_speed * slot_live
    lower_all = face_cells[0]
    upper_all = face_cells[1]
    table = halo_blocks[0]
    ext_cells = cdev + 256 * table.shape[1]
    own_hot = (jnp.arange(cdev, dtype=jnp.int32)[:, None] == lower_all[None, :]).astype(jnp.float32)
    up_hot = (jnp.arange(ext_cells, dtype=jnp.int32)[:, None] == upper_all[None, :]).astype(
        jnp.float32
    )
    signed_hot = own_hot - up_hot[:cdev]
    own_twice = jnp.concatenate([own_hot, own_hot], axis=0).astype(jnp.bfloat16)
    up_twice = jnp.concatenate([up_hot, up_hot], axis=0).astype(jnp.bfloat16)
    signed_twice = jnp.concatenate([signed_hot, signed_hot], axis=1).astype(jnp.bfloat16)
    cosine = jnp.cos(theta[:, None] - face_angle[None, :]) * slot_weight[None, :]
    velocity = (group_speed[None, :, None] * cosine[:, None, :]).reshape(dloc * nfreq, fdev)
    forward = jnp.maximum(velocity, 0.0)
    backward = jnp.minimum(velocity, 0.0)
    requests = with_halo(halo_blocks, (("rows", 0),), 1, False)
    wanted_above = requests[2, 0]
    wanted_below = requests[0, 1]
    current = field
    for step in range(ITERS):
        send_up = pick_blocks(current, wanted_above)
        send_down = pick_blocks(current, wanted_below)
        from_below = from_behind(send_up, "rows", 1)
        from_above = from_behind(send_down, "rows", -1)
        extended = jnp.concatenate([current, from_below, from_above], axis=2)
        spectra = extended.reshape(dloc * nfreq, extended.shape[2])
        total = block_flux(
            spectra, cdev, own_twice, up_twice, signed_twice, forward, backward
        )
        moved = current - total.reshape(dloc, nfreq, cdev) * area_scale
        rims = with_halo(moved, (("spec", 0),), 1, True)
        before = rims[:-2]
        after = rims[2:]
        current = (
            moved
            - jnp.maximum(weight_turn, 0.0) * (moved - before)
            - jnp.minimum(weight_turn, 0.0) * (after - moved)
        )
    return current


def solution(mesh):
    return jax.shard_map(
        on_device,
        mesh=mesh,
        in_specs=(
            P("spec", None, "rows"),
            P(),
            P("rows"),
            P("rows"),
            P(None, "rows"),
            P("rows"),
            P("rows", None, None),
            P("rows"),
            P("rows"),
            P("rows"),
        ),
        out_specs=P("spec", None, "rows"),
        check_vma=False,
    )
```

```python
import functools
import math

import jax
import jax.numpy as jnp
from jax import lax
from jax.experimental import pallas as pl
from jax.experimental.pallas import tpu as pltpu
from jax.sharding import PartitionSpec as P

NDIR = 36
ITERS = 3
CHUNKS = 2
FACE_TILE = 256
MESH = pl.DeviceIdType.MESH


def exchange_kernel(mine_ref, all_ref, send_sem, recv_sem):
    count = lax.axis_size("rows")
    me = lax.axis_index("rows")
    barrier = pltpu.get_barrier_semaphore()
    for hop in range(1, count):
        pl.semaphore_signal(
            barrier,
            inc=1,
            device_id={"rows": lax.rem(me + hop, count)},
            device_id_type=MESH,
        )
    pl.semaphore_wait(barrier, count - 1)

    def copy(hop):
        return pltpu.make_async_remote_copy(
            src_ref=mine_ref,
            dst_ref=all_ref.at[hop],
            send_sem=send_sem.at[hop],
            recv_sem=recv_sem.at[hop],
            device_id={"rows": lax.rem(me + hop, count)},
            device_id_type=MESH,
        )

    for hop in range(1, count):
        copy(hop).start()
    all_ref[0] = mine_ref[...]
    for hop in range(1, count):
        copy(hop).wait()


def exchange(block):
    count = lax.axis_size("rows")
    return pl.pallas_call(
        exchange_kernel,
        out_shape=jax.ShapeDtypeStruct((count,) + block.shape, block.dtype),
        in_specs=[pl.BlockSpec(memory_space=pltpu.VMEM)],
        out_specs=pl.BlockSpec(memory_space=pltpu.VMEM),
        scratch_shapes=[
            pltpu.SemaphoreType.DMA((count,)),
            pltpu.SemaphoreType.DMA((count,)),
        ],
        compiler_params=pltpu.CompilerParams(collective_id=0, has_side_effects=True),
    )(block)


def pieces(value):
    high = value.astype(jnp.bfloat16)
    low = (value - high.astype(jnp.float32)).astype(jnp.bfloat16)
    return high, low


def steps_kernel(
    nfreq,
    field_ref,
    lower_row_ref,
    upper_row_ref,
    lower_col_ref,
    upper_col_ref,
    slots_ref,
    cells_ref,
    forward_ref,
    backward_ref,
    gain_ref,
    area_ref,
    turn_ref,
    out_ref,
    current,
    lhs,
    moved,
    own_hot,
    up_hot,
    signed_hot,
    pick_hot,
    flux_sum,
    halo_out,
    halo_in,
    rim_out,
    rim_in,
    halo_send_sem,
    halo_recv_sem,
    rim_send_sem,
    rim_recv_sem,
):
    rows_n = lax.axis_size("rows")
    me = lax.axis_index("rows")
    spec_n = lax.axis_size("spec")
    shard = lax.axis_index("spec")
    prev = lax.rem(shard + spec_n - 1, spec_n)
    following = lax.rem(shard + 1, spec_n)
    _, dloc, fsize, cdev = current.shape
    fdev = own_hot.shape[1]
    rows = dloc * fsize
    width = halo_in.shape[3]
    has_above = me < rows_n - 1
    has_below = me > 0

    barrier = pltpu.get_barrier_semaphore()

    @pl.when(has_above)
    def _():
        pl.semaphore_signal(barrier, inc=1, device_id={"rows": me + 1}, device_id_type=MESH)

    @pl.when(has_below)
    def _():
        pl.semaphore_signal(barrier, inc=1, device_id={"rows": me - 1}, device_id_type=MESH)

    others = (prev,) if spec_n == 2 else (prev, following)
    for other in others:
        pl.semaphore_signal(barrier, inc=1, device_id={"spec": other}, device_id_type=MESH)

    cell_ids = lax.broadcasted_iota(jnp.int32, (cdev, 2 * width), 0)
    pick_hot[...] = jnp.where(cell_ids == cells_ref[...], 1.0, 0.0).astype(jnp.bfloat16)
    for chunk in range(CHUNKS):
        first = chunk * fsize
        here = min(fsize, nfreq - first)
        current[chunk, :, :here, :] = field_ref[:, first : first + here, :]
        if here < fsize:
            current[chunk, :, here:, :] = jnp.zeros((dloc, fsize - here, cdev), jnp.float32)

    row_peers = jnp.where(has_above, 1, 0) + jnp.where(has_below, 1, 0)
    pl.semaphore_wait(barrier, len(others) + row_peers)

    def to_above(turn):
        return pltpu.make_async_remote_copy(
            src_ref=halo_out.at[turn, 0],
            dst_ref=halo_in.at[turn, 0],
            send_sem=halo_send_sem.at[turn, 0],
            recv_sem=halo_recv_sem.at[turn, 0],
            device_id={"rows": me + 1},
            device_id_type=MESH,
        )

    def to_below(turn):
        return pltpu.make_async_remote_copy(
            src_ref=halo_out.at[turn, 1],
            dst_ref=halo_in.at[turn, 1],
            send_sem=halo_send_sem.at[turn, 1],
            recv_sem=halo_recv_sem.at[turn, 1],
            device_id={"rows": me - 1},
            device_id_type=MESH,
        )

    def rim_copy(turn, side):
        return pltpu.make_async_remote_copy(
            src_ref=rim_out.at[turn, side],
            dst_ref=rim_in.at[turn, side],
            send_sem=rim_send_sem.at[turn, side],
            recv_sem=rim_recv_sem.at[turn, side],
            device_id={"spec": following if side == 0 else prev},
            device_id_type=MESH,
        )

    def split_and_send(turn, chunk):
        value = current[chunk].reshape(rows, cdev)
        high, low = pieces(value)
        lhs[chunk, :rows] = high
        lhs[chunk, rows:] = low

        @pl.when(turn < CHUNKS * ITERS)
        def _():
            picked = jnp.dot(lhs[chunk], pick_hot[...], preferred_element_type=jnp.float32)
            total = picked[:rows] + picked[rows:]
            halo_out[turn, 0] = total[:, :width]
            halo_out[turn, 1] = total[:, width:]

            @pl.when(has_above)
            def _():
                to_above(turn).start()

            @pl.when(has_below)
            def _():
                to_below(turn).start()

    def first_send(chunk, carry):
        split_and_send(chunk, chunk)
        return carry

    lax.fori_loop(0, CHUNKS, first_send, 0)

    @pl.when(jnp.logical_not(has_below))
    def _():
        for turn in range(CHUNKS * ITERS):
            halo_in[turn, 0] = jnp.zeros((rows, width), jnp.float32)

    @pl.when(jnp.logical_not(has_above))
    def _():
        for turn in range(CHUNKS * ITERS):
            halo_in[turn, 1] = jnp.zeros((rows, width), jnp.float32)

    def one_hot(mask):
        return jnp.where(mask, 1.0, 0.0)

    for tile in range(fdev // FACE_TILE):
        faces = pl.ds(tile * FACE_TILE, FACE_TILE)
        ids = lax.broadcasted_iota(jnp.int32, (cdev, FACE_TILE), 0)
        own_hot[:, faces] = one_hot(ids == lower_row_ref[:, faces]).astype(jnp.bfloat16)
        up_hot[:cdev, faces] = one_hot(ids == upper_row_ref[:, faces]).astype(jnp.bfloat16)
        up_hot[cdev:, faces] = one_hot(slots_ref[...] == upper_row_ref[:, faces]).astype(
            jnp.bfloat16
        )
        lanes = lax.broadcasted_iota(jnp.int32, (FACE_TILE, cdev), 1)
        signed_hot[faces, :] = (
            one_hot(lanes == lower_col_ref[faces, :]) - one_hot(lanes == upper_col_ref[faces, :])
        ).astype(jnp.bfloat16)

    turn_rate = turn_ref[...]
    ahead = jnp.maximum(turn_rate, 0.0)
    back = jnp.minimum(turn_rate, 0.0)

    def one_turn(turn, carry):
        chunk = lax.rem(turn, CHUNKS)

        @pl.when(has_below)
        def _():
            to_above(turn).wait_recv()

        @pl.when(has_above)
        def _():
            to_below(turn).wait_recv()

        halos = []
        for side in range(2):
            high, low = pieces(halo_in[turn, side])
            halos.append(jnp.concatenate([high, low], axis=0))
        halo = jnp.concatenate(halos, axis=1)
        flux_sum[...] = jnp.zeros_like(flux_sum)

        def face_tile(tile, inner):
            faces = pl.ds(pl.multiple_of(tile * FACE_TILE, FACE_TILE), FACE_TILE)
            own = lhs[chunk]
            low_vals = jnp.dot(own, own_hot[:, faces], preferred_element_type=jnp.float32)
            up_vals = jnp.dot(own, up_hot[:cdev, faces], preferred_element_type=jnp.float32)
            up_vals += jnp.dot(halo, up_hot[cdev:, faces], preferred_element_type=jnp.float32)
            low_vals = (low_vals[:rows] + low_vals[rows:]).reshape(dloc, fsize, FACE_TILE)
            up_vals = (up_vals[:rows] + up_vals[rows:]).reshape(dloc, fsize, FACE_TILE)
            flux = forward_ref[:, :, faces] * low_vals + backward_ref[:, :, faces] * up_vals
            high, low = pieces(flux.reshape(rows, FACE_TILE))
            both = jnp.concatenate([high, low], axis=0)
            flux_sum[...] += jnp.dot(
                both, signed_hot[faces, :], preferred_element_type=jnp.float32
            )
            return inner

        lax.fori_loop(0, fdev // FACE_TILE, face_tile, 0)
        total = (flux_sum[:rows] + flux_sum[rows:]).reshape(dloc, fsize, cdev)
        scale = gain_ref[chunk] * area_ref[...]
        moved[...] = current[chunk] - total * scale[None]
        rim_out[turn, 0] = moved[dloc - 1]
        rim_out[turn, 1] = moved[0]
        rim_copy(turn, 0).start()
        rim_copy(turn, 1).start()
        mid = moved[1 : dloc - 1]
        current[chunk, 1 : dloc - 1] = (
            mid - ahead * (mid - moved[: dloc - 2]) - back * (moved[2:] - mid)
        )
        rim_copy(turn, 0).wait_recv()
        rim_copy(turn, 1).wait_recv()
        edge = moved[0]
        current[chunk, 0] = edge - ahead * (edge - rim_in[turn, 0]) - back * (moved[1] - edge)
        edge = moved[dloc - 1]
        current[chunk, dloc - 1] = (
            edge - ahead * (edge - moved[dloc - 2]) - back * (rim_in[turn, 1] - edge)
        )
        split_and_send(turn + CHUNKS, chunk)
        return carry

    lax.fori_loop(0, CHUNKS * ITERS, one_turn, 0)

    for chunk in range(CHUNKS):
        first = chunk * fsize
        here = min(fsize, nfreq - first)
        out_ref[:, first : first + here, :] = current[chunk, :, :here, :]

    def drain(turn, carry):
        rim_copy(turn, 0).wait_send()
        rim_copy(turn, 1).wait_send()

        @pl.when(has_above)
        def _():
            to_above(turn).wait_send()

        @pl.when(has_below)
        def _():
            to_below(turn).wait_send()

        return carry

    lax.fori_loop(0, CHUNKS * ITERS, drain, 0)


def run_steps(collective_id, width, slots, cells, field, faces, forward, backward, gain, area, turn):
    dloc, nfreq, cdev = field.shape
    fdev = faces.shape[1]
    fsize = gain.shape[1]
    rows = dloc * fsize
    turns = CHUNKS * ITERS
    vmem = pl.BlockSpec(memory_space=pltpu.VMEM)
    operands = (
        field,
        faces[0:1],
        faces[1:2],
        faces[0][:, None],
        faces[1][:, None],
        slots,
        cells,
        forward[:, None, :],
        backward[:, None, :],
        gain,
        area[None, :],
        turn[None, :],
    )
    return pl.pallas_call(
        functools.partial(steps_kernel, nfreq),
        out_shape=jax.ShapeDtypeStruct(field.shape, jnp.float32),
        in_specs=[vmem] * len(operands),
        out_specs=vmem,
        scratch_shapes=[
            pltpu.VMEM((CHUNKS, dloc, fsize, cdev), jnp.float32),
            pltpu.VMEM((CHUNKS, 2 * rows, cdev), jnp.bfloat16),
            pltpu.VMEM((dloc, fsize, cdev), jnp.float32),
            pltpu.VMEM((cdev, fdev), jnp.bfloat16),
            pltpu.VMEM((cdev + 2 * width, fdev), jnp.bfloat16),
            pltpu.VMEM((fdev, cdev), jnp.bfloat16),
            pltpu.VMEM((cdev, 2 * width), jnp.bfloat16),
            pltpu.VMEM((2 * rows, cdev), jnp.float32),
            pltpu.VMEM((turns, 2, rows, width), jnp.float32),
            pltpu.VMEM((turns, 2, rows, width), jnp.float32),
            pltpu.VMEM((turns, 2, fsize, cdev), jnp.float32),
            pltpu.VMEM((turns, 2, fsize, cdev), jnp.float32),
            pltpu.SemaphoreType.DMA((turns, 2)),
            pltpu.SemaphoreType.DMA((turns, 2)),
            pltpu.SemaphoreType.DMA((turns, 2)),
            pltpu.SemaphoreType.DMA((turns, 2)),
        ],
        compiler_params=pltpu.CompilerParams(
            collective_id=collective_id, has_side_effects=True, vmem_limit_bytes=60 * 2**20
        ),
    )(*operands)


def on_device(
    field,
    group_speed,
    face_angle,
    face_speed,
    face_cells,
    face_live,
    halo_blocks,
    cell_level,
    polar_mask,
    turn_rate,
):
    dloc, nfreq, cdev = field.shape
    fdev = face_angle.shape[0]
    rows_n = lax.axis_size("rows")
    me = lax.axis_index("rows")
    first_dir = lax.axis_index("spec") * dloc
    theta = ((first_dir + jnp.arange(dloc, dtype=jnp.int32)).astype(jnp.float32) + 0.5) * (
        2.0 * math.pi / NDIR
    )
    turn = polar_mask.astype(jnp.float32) * turn_rate
    area = jnp.exp2(-cell_level.astype(jnp.float32))
    live = jnp.arange(fdev, dtype=jnp.int32) < face_live[0] * 128
    slot_weight = face_speed * live.astype(jnp.float32)
    cosine = jnp.cos(theta[:, None] - face_angle[None, :]) * slot_weight[None, :]
    forward = jnp.maximum(cosine, 0.0)
    backward = jnp.minimum(cosine, 0.0)
    fsize = 8 * (-(-nfreq // (8 * CHUNKS)))
    gain = jnp.pad(group_speed, (0, CHUNKS * fsize - nfreq)).reshape(CHUNKS, fsize, 1)

    table = halo_blocks[0]
    full = 128 * table.shape[1]
    half = full // 2
    spots = jnp.arange(2 * full, dtype=jnp.int32)
    asked = jnp.any(
        (spots[:, None] + cdev == face_cells[1][None, :]) & live[None, :], axis=1
    ).reshape(2, full)
    spot = jnp.arange(full, dtype=jnp.int32)
    rank = jnp.sum(
        jnp.where(asked[:, None, :] & (spot[None, None, :] < spot[None, :, None]), 1, 0), axis=2
    )
    cells_full = (table[:, :, None] * 128 + jnp.arange(128, dtype=jnp.int32)).reshape(2, full)
    slots_full = cdev + spots.reshape(2, full)
    order = jnp.arange(half, dtype=jnp.int32)
    hit = asked[:, None, :] & (rank[:, None, :] == order[None, :, None])
    cells_half = jnp.sum(jnp.where(hit, cells_full[:, None, :] + 1, 0), axis=2) - 1
    slots_half = jnp.sum(jnp.where(hit, slots_full[:, None, :] + 1, 0), axis=2) - 1
    most = jnp.max(jnp.sum(asked.astype(jnp.int32), axis=1))
    width = max(full, 128)
    block = jnp.stack(
        [jnp.pad(cells_half[side], (0, width - half)) for side in range(2)]
        + [cells_full[0], cells_full[1], jnp.full((width,), most)]
    )
    block = jnp.pad(block, ((0, 8 - block.shape[0]), (0, 0)))
    lists = exchange(block)
    fits = jnp.max(lists[:, 4, 0]) <= half
    from_below = lists[1]
    from_above = lists[rows_n - 1]
    shared = (field, face_cells, forward, backward, gain, area, turn)

    def narrow(args):
        cells = jnp.concatenate([from_above[0, :half], from_below[1, :half]])[None, :]
        return run_steps(1, half, slots_half.reshape(-1, 1), cells, *args)

    def wide(args):
        cells = jnp.concatenate([from_above[2], from_below[3]])[None, :]
        return run_steps(2, full, slots_full.reshape(-1, 1), cells, *args)

    return lax.cond(fits, narrow, wide, shared)


def solution(mesh):
    return jax.shard_map(
        on_device,
        mesh=mesh,
        in_specs=(
            P("spec", None, "rows"),
            P(),
            P("rows"),
            P("rows"),
            P(None, "rows"),
            P("rows"),
            P("rows", None, None),
            P("rows"),
            P("rows"),
            P("rows"),
        ),
        out_specs=P("spec", None, "rows"),
        check_vma=False,
    )
```

```python
import functools
import math

import jax
import jax.numpy as jnp
from jax import lax
from jax.experimental import pallas as pl
from jax.experimental.pallas import tpu as pltpu
from jax.sharding import PartitionSpec as P

NDIR = 36
ITERS = 3
CHUNKS = 2
FACE_TILE = 256
MESH = pl.DeviceIdType.MESH


def exchange_kernel(
    cdev,
    half,
    faces_ref,
    live_ref,
    table_ref,
    cells_ref,
    slots_ref,
    most_ref,
    above_ref,
    below_ref,
    mine,
    every,
    send_sem,
    recv_sem,
):
    count = lax.axis_size("rows")
    me = lax.axis_index("rows")
    barrier = pltpu.get_barrier_semaphore()
    for hop in range(1, count):
        pl.semaphore_signal(
            barrier,
            inc=1,
            device_id={"rows": lax.rem(me + hop, count)},
            device_id_type=MESH,
        )

    fdev = faces_ref.shape[1]
    blocks = table_ref.shape[2]
    full = 128 * blocks
    face = lax.broadcasted_iota(jnp.int32, (1, fdev), 1)
    upper = jnp.where(face < live_ref[0] * 128, faces_ref[1:2, :], -1)
    below_diagonal = lax.broadcasted_iota(jnp.int32, (full, full), 1) < lax.broadcasted_iota(
        jnp.int32, (full, full), 0
    )
    triangle = jnp.where(below_diagonal, 1.0, 0.0).astype(jnp.bfloat16)
    spot = lax.broadcasted_iota(jnp.int32, (full, half), 0)
    order = lax.broadcasted_iota(jnp.int32, (full, half), 1).astype(jnp.float32)
    mine[...] = jnp.zeros_like(mine)
    most = jnp.zeros((1, half), jnp.float32)
    for side in range(2):
        base = cdev + side * full
        spots = lax.broadcasted_iota(jnp.int32, (full, fdev), 0) + base
        asked = jnp.max(jnp.where(spots == upper, 1.0, 0.0), axis=1, keepdims=True)
        asked = jnp.broadcast_to(asked, (full, half))
        rank = jnp.dot(triangle, asked.astype(jnp.bfloat16), preferred_element_type=jnp.float32)
        hit = jnp.where(rank == order, asked, 0.0)
        cell = spot
        for k in range(blocks):
            inside = (spot >= 128 * k) & (spot < 128 * (k + 1))
            cell = jnp.where(inside, table_ref[0, side, k] * 128 + spot - 128 * k, cell)
            row = 3 + side * blocks + k
            mine[row : row + 1, :] = jnp.full((1, half), table_ref[0, side, k], jnp.int32)

        def listed(values):
            total = jnp.sum(hit * (values + 1).astype(jnp.float32), axis=0, keepdims=True)
            return total.astype(jnp.int32) - 1

        mine[side : side + 1, :] = listed(cell)
        slots_ref[:, side * half : (side + 1) * half] = listed(spot + base)
        most = jnp.maximum(most, jnp.sum(asked, axis=0, keepdims=True))
    mine[2:3, :] = most.astype(jnp.int32)

    pl.semaphore_wait(barrier, count - 1)

    def copy(hop):
        return pltpu.make_async_remote_copy(
            src_ref=mine,
            dst_ref=every.at[hop],
            send_sem=send_sem.at[hop],
            recv_sem=recv_sem.at[hop],
            device_id={"rows": lax.rem(me + hop, count)},
            device_id_type=MESH,
        )

    for hop in range(1, count):
        copy(hop).start()
    highest = mine[2:3, :]
    for hop in range(1, count):
        copy(hop).wait()
        highest = jnp.maximum(highest, every[hop, 2:3, :])
    most_ref[...] = highest
    above_ref[...] = every[count - 1]
    below_ref[...] = every[1]
    cells_ref[:, :half] = every[count - 1, 0:1, :]
    cells_ref[:, half:] = every[1, 1:2, :]


def exchange(cdev, half, faces, live, table):
    count = lax.axis_size("rows")
    vmem = pl.BlockSpec(memory_space=pltpu.VMEM)
    smem = pl.BlockSpec(memory_space=pltpu.SMEM)
    height = 8 * (-(-(3 + 2 * table.shape[2]) // 8))
    shapes = ((1, 2 * half), (1, 2 * half), (1, half), (height, half), (height, half))
    return pl.pallas_call(
        functools.partial(exchange_kernel, cdev, half),
        out_shape=[jax.ShapeDtypeStruct(shape, jnp.int32) for shape in shapes],
        in_specs=[vmem, smem, smem],
        out_specs=[vmem] * len(shapes),
        scratch_shapes=[
            pltpu.VMEM((height, half), jnp.int32),
            pltpu.VMEM((count, height, half), jnp.int32),
            pltpu.SemaphoreType.DMA((count,)),
            pltpu.SemaphoreType.DMA((count,)),
        ],
        compiler_params=pltpu.CompilerParams(collective_id=0, has_side_effects=True),
    )(faces, live, table)


def pieces(value):
    high = value.astype(jnp.bfloat16)
    low = (value - high.astype(jnp.float32)).astype(jnp.bfloat16)
    return high, low


def steps_kernel(
    nfreq,
    field_ref,
    faces_ref,
    slots_ref,
    cells_ref,
    cosine_ref,
    group_speed_ref,
    level_ref,
    mask_ref,
    rate_ref,
    out_ref,
    forward_ref,
    backward_ref,
    scale_ref,
    current,
    lhs,
    moved,
    own_hot,
    up_hot,
    signed_hot,
    pick_hot,
    flux_sum,
    halo_out,
    halo_in,
    rim_out,
    rim_in,
    halo_send_sem,
    halo_recv_sem,
    rim_send_sem,
    rim_recv_sem,
):
    rows_n = lax.axis_size("rows")
    me = lax.axis_index("rows")
    spec_n = lax.axis_size("spec")
    shard = lax.axis_index("spec")
    prev = lax.rem(shard + spec_n - 1, spec_n)
    following = lax.rem(shard + 1, spec_n)
    _, dloc, fsize, cdev = current.shape
    fdev = own_hot.shape[1]
    rows = dloc * fsize
    width = halo_in.shape[4]
    has_above = me < rows_n - 1
    has_below = me > 0

    barrier = pltpu.get_barrier_semaphore()

    @pl.when(has_above)
    def _():
        pl.semaphore_signal(barrier, inc=1, device_id={"rows": me + 1}, device_id_type=MESH)

    @pl.when(has_below)
    def _():
        pl.semaphore_signal(barrier, inc=1, device_id={"rows": me - 1}, device_id_type=MESH)

    others = (prev,) if spec_n == 2 else (prev, following)
    for other in others:
        pl.semaphore_signal(barrier, inc=1, device_id={"spec": other}, device_id_type=MESH)

    cell_ids = lax.broadcasted_iota(jnp.int32, (cdev, 2 * width), 0)
    pick_hot[...] = jnp.where(cell_ids == cells_ref[...], 1.0, 0.0).astype(jnp.bfloat16)
    for chunk in range(CHUNKS):
        first = chunk * fsize
        here = min(fsize, nfreq - first)
        current[chunk, :, :here, :] = field_ref[:, first : first + here, :]
        if here < fsize:
            current[chunk, :, here:, :] = jnp.zeros((dloc, fsize - here, cdev), jnp.float32)

    def kept(chunk):
        return pl.ds(0, fsize)

    def to_above(turn, chunk):
        return pltpu.make_async_remote_copy(
            src_ref=halo_out.at[turn, 0, :, kept(chunk), :],
            dst_ref=halo_in.at[turn, 0, :, kept(chunk), :],
            send_sem=halo_send_sem.at[turn, 0],
            recv_sem=halo_recv_sem.at[turn, 0],
            device_id={"rows": me + 1},
            device_id_type=MESH,
        )

    def to_below(turn, chunk):
        return pltpu.make_async_remote_copy(
            src_ref=halo_out.at[turn, 1, :, kept(chunk), :],
            dst_ref=halo_in.at[turn, 1, :, kept(chunk), :],
            send_sem=halo_send_sem.at[turn, 1],
            recv_sem=halo_recv_sem.at[turn, 1],
            device_id={"rows": me - 1},
            device_id_type=MESH,
        )

    def rim_copy(turn, side):
        return pltpu.make_async_remote_copy(
            src_ref=rim_out.at[turn, side],
            dst_ref=rim_in.at[turn, side],
            send_sem=rim_send_sem.at[turn, side],
            recv_sem=rim_recv_sem.at[turn, side],
            device_id={"spec": following if side == 0 else prev},
            device_id_type=MESH,
        )

    def split(chunk):
        high, low = pieces(current[chunk].reshape(rows, cdev))
        lhs[chunk, :rows] = high
        lhs[chunk, rows:] = low

    def pick(turn, chunk):
        picked = jnp.dot(lhs[chunk], pick_hot[...], preferred_element_type=jnp.float32)
        total = (picked[:rows] + picked[rows:]).reshape(dloc, fsize, 2 * width)
        halo_out[turn, 0] = total[:, :, :width]
        halo_out[turn, 1] = total[:, :, width:]

    def send(turn, chunk):
        @pl.when(has_above)
        def _():
            to_above(turn, chunk).start()

        @pl.when(has_below)
        def _():
            to_below(turn, chunk).start()

    for chunk in range(CHUNKS):
        split(chunk)
        pick(chunk, chunk)
        if chunk == 0:
            row_peers = jnp.where(has_above, 1, 0) + jnp.where(has_below, 1, 0)
            pl.semaphore_wait(barrier, len(others) + row_peers)
        send(chunk, chunk)

    @pl.when(jnp.logical_not(has_below))
    def _():
        for turn in range(CHUNKS * ITERS):
            halo_in[turn, 0] = jnp.zeros((dloc, fsize, width), jnp.float32)

    @pl.when(jnp.logical_not(has_above))
    def _():
        for turn in range(CHUNKS * ITERS):
            halo_in[turn, 1] = jnp.zeros((dloc, fsize, width), jnp.float32)

    def one_hot(mask):
        return jnp.where(mask, 1.0, 0.0)

    def as_column(row):
        return jnp.transpose(jnp.broadcast_to(row, (128, row.shape[1])))

    slot_column = as_column(slots_ref[...])
    for lane in range(fdev // 128):
        faces = pl.ds(lane * 128, 128)
        ids = lax.broadcasted_iota(jnp.int32, (cdev, 128), 0)
        lower = faces_ref[0:1, faces]
        upper = faces_ref[1:2, faces]
        own_hot[:, faces] = one_hot(ids == lower).astype(jnp.bfloat16)
        up_hot[:cdev, faces] = one_hot(ids == upper).astype(jnp.bfloat16)
        up_hot[cdev:, faces] = one_hot(slot_column == upper).astype(jnp.bfloat16)
        lower = as_column(lower)
        upper = as_column(upper)
        for part in range(cdev // 128):
            lanes = lax.broadcasted_iota(jnp.int32, (128, 128), 1) + part * 128
            signed_hot[faces, part * 128 : (part + 1) * 128] = (
                one_hot(lanes == lower) - one_hot(lanes == upper)
            ).astype(jnp.bfloat16)
    for d in range(dloc):
        forward_ref[d] = jnp.maximum(cosine_ref[d : d + 1, :], 0.0)
        backward_ref[d] = jnp.minimum(cosine_ref[d : d + 1, :], 0.0)
    area = 1.0 / lax.shift_left(jnp.ones_like(level_ref[...]), level_ref[...]).astype(jnp.float32)
    scale_ref[...] = jnp.zeros_like(scale_ref)
    for f in range(nfreq):
        at = f % fsize
        scale_ref[f // fsize, at : at + 1, :] = group_speed_ref[f] * area

    turn_rate = mask_ref[...].astype(jnp.float32) * rate_ref[...]
    ahead = jnp.maximum(turn_rate, 0.0)
    back = jnp.minimum(turn_rate, 0.0)

    def one_turn(step, chunk):
        turn = step * CHUNKS + chunk

        @pl.when(has_below)
        def _():
            to_above(turn, chunk).wait_recv()

        @pl.when(has_above)
        def _():
            to_below(turn, chunk).wait_recv()

        halos = []
        for side in range(2):
            high, low = pieces(halo_in[turn, side].reshape(rows, width))
            halos.append(jnp.concatenate([high, low], axis=0))
        halo = jnp.concatenate(halos, axis=1)
        flux_sum[...] = jnp.zeros_like(flux_sum)

        def face_tile(tile, inner):
            faces = pl.ds(pl.multiple_of(tile * FACE_TILE, FACE_TILE), FACE_TILE)
            own = lhs[chunk]
            low_vals = jnp.dot(own, own_hot[:, faces], preferred_element_type=jnp.float32)
            up_vals = jnp.dot(own, up_hot[:cdev, faces], preferred_element_type=jnp.float32)
            up_vals += jnp.dot(halo, up_hot[cdev:, faces], preferred_element_type=jnp.float32)
            low_vals = (low_vals[:rows] + low_vals[rows:]).reshape(dloc, fsize, FACE_TILE)
            up_vals = (up_vals[:rows] + up_vals[rows:]).reshape(dloc, fsize, FACE_TILE)
            flux = forward_ref[:, :, faces] * low_vals + backward_ref[:, :, faces] * up_vals
            high, low = pieces(flux.reshape(rows, FACE_TILE))
            both = jnp.concatenate([high, low], axis=0)
            flux_sum[...] += jnp.dot(
                both, signed_hot[faces, :], preferred_element_type=jnp.float32
            )
            return inner

        lax.fori_loop(0, fdev // FACE_TILE, face_tile, 0)
        total = (flux_sum[:rows] + flux_sum[rows:]).reshape(dloc, fsize, cdev)
        moved[...] = current[chunk] - total * scale_ref[chunk]
        rim_out[turn, 0] = moved[dloc - 1]
        rim_out[turn, 1] = moved[0]
        rim_copy(turn, 0).start()
        rim_copy(turn, 1).start()
        mid = moved[1 : dloc - 1]
        current[chunk, 1 : dloc - 1] = (
            mid - ahead * (mid - moved[: dloc - 2]) - back * (moved[2:] - mid)
        )
        rim_copy(turn, 0).wait_recv()
        rim_copy(turn, 1).wait_recv()
        edge = moved[0]
        current[chunk, 0] = edge - ahead * (edge - rim_in[turn, 0]) - back * (moved[1] - edge)
        edge = moved[dloc - 1]
        current[chunk, dloc - 1] = (
            edge - ahead * (edge - moved[dloc - 2]) - back * (rim_in[turn, 1] - edge)
        )

        @pl.when(step < ITERS - 1)
        def _():
            split(chunk)
            pick(turn + CHUNKS, chunk)
            send(turn + CHUNKS, chunk)

    def one_step(step, carry):
        for chunk in range(CHUNKS):
            one_turn(step, chunk)
        return carry

    lax.fori_loop(0, ITERS, one_step, 0)

    for chunk in range(CHUNKS):
        first = chunk * fsize
        here = min(fsize, nfreq - first)
        out_ref[:, first : first + here, :] = current[chunk, :, :here, :]

    def drain(step, carry):
        for chunk in range(CHUNKS):
            turn = step * CHUNKS + chunk
            rim_copy(turn, 0).wait_send()
            rim_copy(turn, 1).wait_send()

            @pl.when(has_above)
            def _(turn=turn, chunk=chunk):
                to_above(turn, chunk).wait_send()

            @pl.when(has_below)
            def _(turn=turn, chunk=chunk):
                to_below(turn, chunk).wait_send()

        return carry

    lax.fori_loop(0, ITERS, drain, 0)


def run_steps(collective_id, width, slots, cells, *rest):
    field, faces, cosine, group_speed, level, mask, rate = rest
    dloc, nfreq, cdev = field.shape
    fdev = faces.shape[1]
    fsize = 8 * (-(-nfreq // (8 * CHUNKS)))
    rows = dloc * fsize
    turns = CHUNKS * ITERS
    vmem = pl.BlockSpec(memory_space=pltpu.VMEM)
    smem = pl.BlockSpec(memory_space=pltpu.SMEM)
    operands = (field, faces, slots, cells, cosine, group_speed, level, mask, rate)
    return pl.pallas_call(
        functools.partial(steps_kernel, nfreq),
        out_shape=jax.ShapeDtypeStruct(field.shape, jnp.float32),
        in_specs=[vmem] * 5 + [smem] + [vmem] * 3,
        out_specs=vmem,
        scratch_shapes=[
            pltpu.VMEM((dloc, 1, fdev), jnp.float32),
            pltpu.VMEM((dloc, 1, fdev), jnp.float32),
            pltpu.VMEM((CHUNKS, fsize, cdev), jnp.float32),
            pltpu.VMEM((CHUNKS, dloc, fsize, cdev), jnp.float32),
            pltpu.VMEM((CHUNKS, 2 * rows, cdev), jnp.bfloat16),
            pltpu.VMEM((dloc, fsize, cdev), jnp.float32),
            pltpu.VMEM((cdev, fdev), jnp.bfloat16),
            pltpu.VMEM((cdev + 2 * width, fdev), jnp.bfloat16),
            pltpu.VMEM((fdev, cdev), jnp.bfloat16),
            pltpu.VMEM((cdev, 2 * width), jnp.bfloat16),
            pltpu.VMEM((2 * rows, cdev), jnp.float32),
            pltpu.VMEM((turns, 2, dloc, fsize, width), jnp.float32),
            pltpu.VMEM((turns, 2, dloc, fsize, width), jnp.float32),
            pltpu.VMEM((turns, 2, fsize, cdev), jnp.float32),
            pltpu.VMEM((turns, 2, fsize, cdev), jnp.float32),
            pltpu.SemaphoreType.DMA((turns, 2)),
            pltpu.SemaphoreType.DMA((turns, 2)),
            pltpu.SemaphoreType.DMA((turns, 2)),
            pltpu.SemaphoreType.DMA((turns, 2)),
        ],
        compiler_params=pltpu.CompilerParams(
            collective_id=collective_id, has_side_effects=True, vmem_limit_bytes=60 * 2**20
        ),
    )(*operands)


def on_device(
    field,
    group_speed,
    face_angle,
    face_speed,
    face_cells,
    face_live,
    halo_blocks,
    cell_level,
    polar_mask,
    turn_rate,
):
    dloc, nfreq, cdev = field.shape
    fdev = face_angle.shape[0]
    first_dir = lax.axis_index("spec") * dloc
    theta = ((first_dir + jnp.arange(dloc, dtype=jnp.int32)).astype(jnp.float32) + 0.5) * (
        2.0 * math.pi / NDIR
    )
    live = jnp.arange(fdev, dtype=jnp.int32) < face_live[0] * 128
    slot_weight = face_speed * live.astype(jnp.float32)
    cosine = jnp.cos(theta[:, None] - face_angle[None, :]) * slot_weight[None, :]
    blocks = halo_blocks.shape[2]
    full = 128 * blocks
    half = full // 2
    cells, slots, most, above, below = exchange(cdev, half, face_cells, face_live, halo_blocks)
    fits = most[0, 0] <= half
    shared = (
        field,
        face_cells,
        cosine,
        group_speed,
        cell_level[None, :],
        polar_mask[None, :],
        turn_rate[None, :],
    )

    def narrow(args):
        return run_steps(1, half, slots, cells, *args)

    def wide(args):
        tables = jnp.concatenate([above[3 : 3 + blocks, 0], below[3 + blocks : 3 + 2 * blocks, 0]])
        every_cell = tables[:, None] * 128 + jnp.arange(128, dtype=jnp.int32)
        every_slot = cdev + jnp.arange(2 * full, dtype=jnp.int32)
        return run_steps(2, full, every_slot[None, :], every_cell.reshape(1, -1), *args)

    return lax.cond(fits, narrow, wide, shared)


def solution(mesh):
    return jax.shard_map(
        on_device,
        mesh=mesh,
        in_specs=(
            P("spec", None, "rows"),
            P(),
            P("rows"),
            P("rows"),
            P(None, "rows"),
            P("rows"),
            P("rows", None, None),
            P("rows"),
            P("rows"),
            P("rows"),
        ),
        out_specs=P("spec", None, "rows"),
        check_vma=False,
    )
```

```python
import functools
import math

import jax
import jax.numpy as jnp
from jax import lax
from jax.experimental import pallas as pl
from jax.experimental.pallas import tpu as pltpu
from jax.sharding import PartitionSpec as P

NDIR = 36
ITERS = 3
CHUNKS = 2
FACE_TILE = 512
MESH = pl.DeviceIdType.MESH


def exchange_kernel(
    cdev,
    half,
    faces_ref,
    live_ref,
    table_ref,
    cells_ref,
    slots_ref,
    most_ref,
    above_ref,
    below_ref,
    mine,
    every,
    send_sem,
    recv_sem,
):
    count = lax.axis_size("rows")
    me = lax.axis_index("rows")
    barrier = pltpu.get_barrier_semaphore()
    for hop in range(1, count):
        pl.semaphore_signal(
            barrier,
            inc=1,
            device_id={"rows": lax.rem(me + hop, count)},
            device_id_type=MESH,
        )

    fdev = faces_ref.shape[1]
    blocks = table_ref.shape[2]
    full = 128 * blocks
    face = lax.broadcasted_iota(jnp.int32, (1, fdev), 1)
    upper = jnp.where(face < live_ref[0] * 128, faces_ref[1:2, :], -1)
    below_diagonal = lax.broadcasted_iota(jnp.int32, (full, full), 1) < lax.broadcasted_iota(
        jnp.int32, (full, full), 0
    )
    triangle = jnp.where(below_diagonal, 1.0, 0.0).astype(jnp.bfloat16)
    spot = lax.broadcasted_iota(jnp.int32, (full, half), 0)
    order = lax.broadcasted_iota(jnp.int32, (full, half), 1).astype(jnp.float32)
    mine[...] = jnp.zeros_like(mine)
    most = jnp.zeros((1, half), jnp.float32)
    for side in range(2):
        base = cdev + side * full
        spots = lax.broadcasted_iota(jnp.int32, (full, fdev), 0) + base
        asked = jnp.max(jnp.where(spots == upper, 1.0, 0.0), axis=1, keepdims=True)
        asked = jnp.broadcast_to(asked, (full, half))
        rank = jnp.dot(triangle, asked.astype(jnp.bfloat16), preferred_element_type=jnp.float32)
        hit = jnp.where(rank == order, asked, 0.0)
        cell = spot
        for k in range(blocks):
            inside = (spot >= 128 * k) & (spot < 128 * (k + 1))
            cell = jnp.where(inside, table_ref[0, side, k] * 128 + spot - 128 * k, cell)
            row = 3 + side * blocks + k
            mine[row : row + 1, :] = jnp.full((1, half), table_ref[0, side, k], jnp.int32)

        def listed(values):
            total = jnp.sum(hit * (values + 1).astype(jnp.float32), axis=0, keepdims=True)
            return total.astype(jnp.int32) - 1

        mine[side : side + 1, :] = listed(cell)
        slots_ref[:, side * half : (side + 1) * half] = listed(spot + base)
        most = jnp.maximum(most, jnp.sum(asked, axis=0, keepdims=True))
    mine[2:3, :] = most.astype(jnp.int32)

    pl.semaphore_wait(barrier, count - 1)

    def copy(hop):
        return pltpu.make_async_remote_copy(
            src_ref=mine,
            dst_ref=every.at[hop],
            send_sem=send_sem.at[hop],
            recv_sem=recv_sem.at[hop],
            device_id={"rows": lax.rem(me + hop, count)},
            device_id_type=MESH,
        )

    for hop in range(1, count):
        copy(hop).start()
    highest = mine[2:3, :]
    for hop in range(1, count):
        copy(hop).wait()
        highest = jnp.maximum(highest, every[hop, 2:3, :])
    most_ref[...] = highest
    above_ref[...] = every[count - 1]
    below_ref[...] = every[1]
    cells_ref[:, :half] = every[count - 1, 0:1, :]
    cells_ref[:, half:] = every[1, 1:2, :]


def exchange(cdev, half, faces, live, table):
    count = lax.axis_size("rows")
    vmem = pl.BlockSpec(memory_space=pltpu.VMEM)
    smem = pl.BlockSpec(memory_space=pltpu.SMEM)
    height = 8 * (-(-(3 + 2 * table.shape[2]) // 8))
    shapes = ((1, 2 * half), (1, 2 * half), (1, half), (height, half), (height, half))
    return pl.pallas_call(
        functools.partial(exchange_kernel, cdev, half),
        out_shape=[jax.ShapeDtypeStruct(shape, jnp.int32) for shape in shapes],
        in_specs=[vmem, smem, smem],
        out_specs=[vmem] * len(shapes),
        scratch_shapes=[
            pltpu.VMEM((height, half), jnp.int32),
            pltpu.VMEM((count, height, half), jnp.int32),
            pltpu.SemaphoreType.DMA((count,)),
            pltpu.SemaphoreType.DMA((count,)),
        ],
        compiler_params=pltpu.CompilerParams(collective_id=0, has_side_effects=True),
    )(faces, live, table)


def pieces(value):
    high = value.astype(jnp.bfloat16)
    low = (value - high.astype(jnp.float32)).astype(jnp.bfloat16)
    return high, low


def steps_kernel(
    nfreq,
    field_ref,
    faces_ref,
    slots_ref,
    cells_ref,
    cosine_ref,
    group_speed_ref,
    level_ref,
    mask_ref,
    rate_ref,
    out_ref,
    forward_ref,
    backward_ref,
    scale_ref,
    current,
    lhs,
    moved,
    own_hot,
    up_hot,
    signed_hot,
    pick_hot,
    flux_sum,
    halo_out,
    halo_in,
    rim_out,
    rim_in,
    halo_send_sem,
    halo_recv_sem,
    rim_send_sem,
    rim_recv_sem,
):
    rows_n = lax.axis_size("rows")
    me = lax.axis_index("rows")
    spec_n = lax.axis_size("spec")
    shard = lax.axis_index("spec")
    prev = lax.rem(shard + spec_n - 1, spec_n)
    following = lax.rem(shard + 1, spec_n)
    _, dloc, fsize, cdev = current.shape
    fdev = own_hot.shape[1]
    rows = dloc * fsize
    width = halo_in.shape[4]
    has_above = me < rows_n - 1
    has_below = me > 0

    barrier = pltpu.get_barrier_semaphore()

    @pl.when(has_above)
    def _():
        pl.semaphore_signal(barrier, inc=1, device_id={"rows": me + 1}, device_id_type=MESH)

    @pl.when(has_below)
    def _():
        pl.semaphore_signal(barrier, inc=1, device_id={"rows": me - 1}, device_id_type=MESH)

    others = (prev,) if spec_n == 2 else (prev, following)
    for other in others:
        pl.semaphore_signal(barrier, inc=1, device_id={"spec": other}, device_id_type=MESH)

    cell_ids = lax.broadcasted_iota(jnp.int32, (cdev, 2 * width), 0)
    pick_hot[...] = jnp.where(cell_ids == cells_ref[...], 1.0, 0.0).astype(jnp.bfloat16)
    for chunk in range(CHUNKS):
        first = chunk * fsize
        here = min(fsize, nfreq - first)
        current[chunk, :, :here, :] = field_ref[:, first : first + here, :]
        if here < fsize:
            current[chunk, :, here:, :] = jnp.zeros((dloc, fsize - here, cdev), jnp.float32)

    def kept(chunk):
        return pl.ds(0, fsize)

    def to_above(turn, chunk):
        return pltpu.make_async_remote_copy(
            src_ref=halo_out.at[turn, 0, :, kept(chunk), :],
            dst_ref=halo_in.at[turn, 0, :, kept(chunk), :],
            send_sem=halo_send_sem.at[turn, 0],
            recv_sem=halo_recv_sem.at[turn, 0],
            device_id={"rows": me + 1},
            device_id_type=MESH,
        )

    def to_below(turn, chunk):
        return pltpu.make_async_remote_copy(
            src_ref=halo_out.at[turn, 1, :, kept(chunk), :],
            dst_ref=halo_in.at[turn, 1, :, kept(chunk), :],
            send_sem=halo_send_sem.at[turn, 1],
            recv_sem=halo_recv_sem.at[turn, 1],
            device_id={"rows": me - 1},
            device_id_type=MESH,
        )

    def rim_copy(turn, side):
        return pltpu.make_async_remote_copy(
            src_ref=rim_out.at[turn, side],
            dst_ref=rim_in.at[turn, side],
            send_sem=rim_send_sem.at[turn, side],
            recv_sem=rim_recv_sem.at[turn, side],
            device_id={"spec": following if side == 0 else prev},
            device_id_type=MESH,
        )

    def split(chunk):
        high, low = pieces(current[chunk].reshape(rows, cdev))
        lhs[chunk, :rows] = high
        lhs[chunk, rows:] = low

    def pick(turn, chunk):
        picked = jnp.dot(lhs[chunk], pick_hot[...], preferred_element_type=jnp.float32)
        total = (picked[:rows] + picked[rows:]).reshape(dloc, fsize, 2 * width)
        halo_out[turn, 0] = total[:, :, :width]
        halo_out[turn, 1] = total[:, :, width:]

    def send(turn, chunk):
        @pl.when(has_above)
        def _():
            to_above(turn, chunk).start()

        @pl.when(has_below)
        def _():
            to_below(turn, chunk).start()

    for chunk in range(CHUNKS):
        split(chunk)
        pick(chunk, chunk)
        if chunk == 0:
            row_peers = jnp.where(has_above, 1, 0) + jnp.where(has_below, 1, 0)
            pl.semaphore_wait(barrier, len(others) + row_peers)
        send(chunk, chunk)

    @pl.when(jnp.logical_not(has_below))
    def _():
        for turn in range(CHUNKS * ITERS):
            halo_in[turn, 0] = jnp.zeros((dloc, fsize, width), jnp.float32)

    @pl.when(jnp.logical_not(has_above))
    def _():
        for turn in range(CHUNKS * ITERS):
            halo_in[turn, 1] = jnp.zeros((dloc, fsize, width), jnp.float32)

    def one_hot(mask):
        return jnp.where(mask, 1.0, 0.0)

    def as_column(row):
        return jnp.transpose(jnp.broadcast_to(row, (128, row.shape[1])))

    slot_column = as_column(slots_ref[...])
    for lane in range(fdev // 128):
        faces = pl.ds(lane * 128, 128)
        ids = lax.broadcasted_iota(jnp.int32, (cdev, 128), 0)
        lower = faces_ref[0:1, faces]
        upper = faces_ref[1:2, faces]
        own_hot[:, faces] = one_hot(ids == lower).astype(jnp.bfloat16)
        up_hot[:cdev, faces] = one_hot(ids == upper).astype(jnp.bfloat16)
        up_hot[cdev:, faces] = one_hot(slot_column == upper).astype(jnp.bfloat16)
        lower = as_column(lower)
        upper = as_column(upper)
        for part in range(cdev // 128):
            lanes = lax.broadcasted_iota(jnp.int32, (128, 128), 1) + part * 128
            signed_hot[faces, part * 128 : (part + 1) * 128] = (
                one_hot(lanes == lower) - one_hot(lanes == upper)
            ).astype(jnp.bfloat16)
    for d in range(dloc):
        forward_ref[d] = jnp.maximum(cosine_ref[d : d + 1, :], 0.0)
        backward_ref[d] = jnp.minimum(cosine_ref[d : d + 1, :], 0.0)
    area = 1.0 / lax.shift_left(jnp.ones_like(level_ref[...]), level_ref[...]).astype(jnp.float32)
    scale_ref[...] = jnp.zeros_like(scale_ref)
    for f in range(nfreq):
        at = f % fsize
        scale_ref[f // fsize, at : at + 1, :] = group_speed_ref[f] * area

    turn_rate = mask_ref[...].astype(jnp.float32) * rate_ref[...]
    ahead = jnp.maximum(turn_rate, 0.0)
    back = jnp.minimum(turn_rate, 0.0)

    def one_turn(step, chunk):
        turn = step * CHUNKS + chunk

        @pl.when(has_below)
        def _():
            to_above(turn, chunk).wait_recv()

        @pl.when(has_above)
        def _():
            to_below(turn, chunk).wait_recv()

        halos = []
        for side in range(2):
            high, low = pieces(halo_in[turn, side].reshape(rows, width))
            halos.append(jnp.concatenate([high, low], axis=0))
        halo = jnp.concatenate(halos, axis=1)
        flux_sum[...] = jnp.zeros_like(flux_sum)

        def face_tile(tile, inner):
            faces = pl.ds(pl.multiple_of(tile * FACE_TILE, FACE_TILE), FACE_TILE)
            own = lhs[chunk]
            low_vals = jnp.dot(own, own_hot[:, faces], preferred_element_type=jnp.float32)
            up_vals = jnp.dot(own, up_hot[:cdev, faces], preferred_element_type=jnp.float32)
            up_vals += jnp.dot(halo, up_hot[cdev:, faces], preferred_element_type=jnp.float32)
            low_vals = (low_vals[:rows] + low_vals[rows:]).reshape(dloc, fsize, FACE_TILE)
            up_vals = (up_vals[:rows] + up_vals[rows:]).reshape(dloc, fsize, FACE_TILE)
            flux = forward_ref[:, :, faces] * low_vals + backward_ref[:, :, faces] * up_vals
            high, low = pieces(flux.reshape(rows, FACE_TILE))
            both = jnp.concatenate([high, low], axis=0)
            flux_sum[...] += jnp.dot(
                both, signed_hot[faces, :], preferred_element_type=jnp.float32
            )
            return inner

        lax.fori_loop(0, fdev // FACE_TILE, face_tile, 0)
        total = (flux_sum[:rows] + flux_sum[rows:]).reshape(dloc, fsize, cdev)
        moved[...] = current[chunk] - total * scale_ref[chunk]
        rim_out[turn, 0] = moved[dloc - 1]
        rim_out[turn, 1] = moved[0]
        rim_copy(turn, 0).start()
        rim_copy(turn, 1).start()
        mid = moved[1 : dloc - 1]
        current[chunk, 1 : dloc - 1] = (
            mid - ahead * (mid - moved[: dloc - 2]) - back * (moved[2:] - mid)
        )
        rim_copy(turn, 0).wait_recv()
        rim_copy(turn, 1).wait_recv()
        edge = moved[0]
        current[chunk, 0] = edge - ahead * (edge - rim_in[turn, 0]) - back * (moved[1] - edge)
        edge = moved[dloc - 1]
        current[chunk, dloc - 1] = (
            edge - ahead * (edge - moved[dloc - 2]) - back * (rim_in[turn, 1] - edge)
        )

        @pl.when(step < ITERS - 1)
        def _():
            split(chunk)
            pick(turn + CHUNKS, chunk)
            send(turn + CHUNKS, chunk)

    def one_step(step, carry):
        for chunk in range(CHUNKS):
            one_turn(step, chunk)
        return carry

    lax.fori_loop(0, ITERS, one_step, 0)

    for chunk in range(CHUNKS):
        first = chunk * fsize
        here = min(fsize, nfreq - first)
        out_ref[:, first : first + here, :] = current[chunk, :, :here, :]

    def drain(step, carry):
        for chunk in range(CHUNKS):
            turn = step * CHUNKS + chunk
            rim_copy(turn, 0).wait_send()
            rim_copy(turn, 1).wait_send()

            @pl.when(has_above)
            def _(turn=turn, chunk=chunk):
                to_above(turn, chunk).wait_send()

            @pl.when(has_below)
            def _(turn=turn, chunk=chunk):
                to_below(turn, chunk).wait_send()

        return carry

    lax.fori_loop(0, ITERS, drain, 0)


def run_steps(collective_id, width, slots, cells, *rest):
    field, faces, cosine, group_speed, level, mask, rate = rest
    dloc, nfreq, cdev = field.shape
    fdev = faces.shape[1]
    fsize = 8 * (-(-nfreq // (8 * CHUNKS)))
    rows = dloc * fsize
    turns = CHUNKS * ITERS
    vmem = pl.BlockSpec(memory_space=pltpu.VMEM)
    smem = pl.BlockSpec(memory_space=pltpu.SMEM)
    operands = (field, faces, slots, cells, cosine, group_speed, level, mask, rate)
    return pl.pallas_call(
        functools.partial(steps_kernel, nfreq),
        out_shape=jax.ShapeDtypeStruct(field.shape, jnp.float32),
        in_specs=[vmem] * 5 + [smem] + [vmem] * 3,
        out_specs=vmem,
        scratch_shapes=[
            pltpu.VMEM((dloc, 1, fdev), jnp.float32),
            pltpu.VMEM((dloc, 1, fdev), jnp.float32),
            pltpu.VMEM((CHUNKS, fsize, cdev), jnp.float32),
            pltpu.VMEM((CHUNKS, dloc, fsize, cdev), jnp.float32),
            pltpu.VMEM((CHUNKS, 2 * rows, cdev), jnp.bfloat16),
            pltpu.VMEM((dloc, fsize, cdev), jnp.float32),
            pltpu.VMEM((cdev, fdev), jnp.bfloat16),
            pltpu.VMEM((cdev + 2 * width, fdev), jnp.bfloat16),
            pltpu.VMEM((fdev, cdev), jnp.bfloat16),
            pltpu.VMEM((cdev, 2 * width), jnp.bfloat16),
            pltpu.VMEM((2 * rows, cdev), jnp.float32),
            pltpu.VMEM((turns, 2, dloc, fsize, width), jnp.float32),
            pltpu.VMEM((turns, 2, dloc, fsize, width), jnp.float32),
            pltpu.VMEM((turns, 2, fsize, cdev), jnp.float32),
            pltpu.VMEM((turns, 2, fsize, cdev), jnp.float32),
            pltpu.SemaphoreType.DMA((turns, 2)),
            pltpu.SemaphoreType.DMA((turns, 2)),
            pltpu.SemaphoreType.DMA((turns, 2)),
            pltpu.SemaphoreType.DMA((turns, 2)),
        ],
        compiler_params=pltpu.CompilerParams(
            collective_id=collective_id, has_side_effects=True, vmem_limit_bytes=60 * 2**20
        ),
    )(*operands)


def on_device(
    field,
    group_speed,
    face_angle,
    face_speed,
    face_cells,
    face_live,
    halo_blocks,
    cell_level,
    polar_mask,
    turn_rate,
):
    dloc, nfreq, cdev = field.shape
    fdev = face_angle.shape[0]
    first_dir = lax.axis_index("spec") * dloc
    theta = ((first_dir + jnp.arange(dloc, dtype=jnp.int32)).astype(jnp.float32) + 0.5) * (
        2.0 * math.pi / NDIR
    )
    live = jnp.arange(fdev, dtype=jnp.int32) < face_live[0] * 128
    slot_weight = face_speed * live.astype(jnp.float32)
    cosine = jnp.cos(theta[:, None] - face_angle[None, :]) * slot_weight[None, :]
    blocks = halo_blocks.shape[2]
    full = 128 * blocks
    half = full // 2
    cells, slots, most, above, below = exchange(cdev, half, face_cells, face_live, halo_blocks)
    fits = most[0, 0] <= half
    shared = (
        field,
        face_cells,
        cosine,
        group_speed,
        cell_level[None, :],
        polar_mask[None, :],
        turn_rate[None, :],
    )

    def narrow(args):
        return run_steps(1, half, slots, cells, *args)

    def wide(args):
        tables = jnp.concatenate([above[3 : 3 + blocks, 0], below[3 + blocks : 3 + 2 * blocks, 0]])
        every_cell = tables[:, None] * 128 + jnp.arange(128, dtype=jnp.int32)
        every_slot = cdev + jnp.arange(2 * full, dtype=jnp.int32)
        return run_steps(2, full, every_slot[None, :], every_cell.reshape(1, -1), *args)

    return lax.cond(fits, narrow, wide, shared)


def solution(mesh):
    return jax.shard_map(
        on_device,
        mesh=mesh,
        in_specs=(
            P("spec", None, "rows"),
            P(),
            P("rows"),
            P("rows"),
            P(None, "rows"),
            P("rows"),
            P("rows", None, None),
            P("rows"),
            P("rows"),
            P("rows"),
        ),
        out_specs=P("spec", None, "rows"),
        check_vma=False,
    )
```
